32 devices in a mesh: dp: 2 (over x), rep: 4 (over y, core), ind: 4 (over z).
Axes of the slice: x: 2, y: 2, z: 4, core: 2. Of those that a mesh axis runs over, the one named last changes fastest.
Arguments:
- points: bfloat16 [6144, 64], P(('dp', 'rep')), may hold values from -6 to 6
- targets: float32 [6144], P(('dp', 'rep')), may hold values from -6 to 6
- inducing: float32 [4096, 64], P('ind'), may hold values from -6 to 6
- whitening: bfloat16 [4096, 4096], P('ind'), may hold values from -0.0546875 to 0.0546875
- mean_v: float32 [4096], P('ind'), may hold values from -12 to 12
- covariance: float32 [4096, 4096], P('ind', ('dp', 'rep')), may hold values from -24 to 24
- precision: float32 [4096, 4096], P('ind', ('dp', 'rep')), may hold values from -3 to 3
- natural_one: float32 [4096], P('ind'), may hold values from -6 to 6
- lengthscales: float32 [64], replicated, may hold values from 1.6 to 24
- hypers: float32 [2], replicated, may hold values from 0.5 to 2
Outputs:
- precision_new: float32 [4096, 4096], P('ind', ('dp', 'rep'))
- natural_new: float32 [4096], P('ind')
- expected_fit: float32 [], replicated
The draws below stay inside these ranges and needn't reach their ends.
All inputs are finite; a program needn't handle non-finite values.
Results may differ from the reference program's by a relative error of at most 0.0076.
Values may be sent and summed in bfloat16 or wider, within the bound.
A program may use at most 128 MiB of HBM per device.

```python
import math
import jax
import jax.numpy as jnp
from jax import lax

M = 4096
F = 64
TOK_DEV = 768
TOKENS = 6144


def block_scale(stream_key, extent, split, least, largest):
    level = 1.0
    for axis_at, parts in split:
        steps = jax.random.uniform(jax.random.fold_in(jax.random.fold_in(stream_key, 6), axis_at), (parts,), jnp.float32, least / len(split), largest / len(split))
        level = level * jnp.repeat(jnp.exp(steps), extent[axis_at] // parts).reshape((-1,) + (1,) * (len(extent) - 1 - axis_at))
    return level


def scatter_about(own_key, extent, scale, most, shards=(), held_as=jnp.bfloat16):
    values = scale * jax.random.normal(own_key, extent, jnp.float32)
    if shards:
        values = values * block_scale(own_key, extent, shards, -0.22, 0.18)
    return jnp.clip(values, -most, most).astype(held_as)


def setup_inputs(seed: int = 0) -> dict:
    seeds = jax.random.split(jax.random.key(seed), 11)
    return {
        "points": scatter_about(seeds[0], (TOKENS, F), 1.0, 6.0, ((0, 8),)),
        "targets": scatter_about(seeds[1], (TOKENS,), 1.0, 6.0, ((0, 8),), jnp.float32),
        "inducing": scatter_about(seeds[2], (M, F), 1.0, 6.0, ((0, 4),), jnp.float32),
        "whitening": scatter_about(seeds[3], (M, M), (TOKENS * M // 2048) ** -0.5, 0.0546875, ((0, 4),)),
        "mean_v": scatter_about(seeds[4], (M,), 2.0, 12.0, ((0, 4),), jnp.float32),
        "covariance": scatter_about(seeds[5], (M, M), 4.0, 24.0, ((0, 4), (1, 8)), jnp.float32),
        "precision": scatter_about(seeds[6], (M, M), 0.5, 3.0, ((0, 4), (1, 8)), jnp.float32),
        "natural_one": scatter_about(seeds[7], (M,), 1.0, 6.0, ((0, 4),), jnp.float32),
        "lengthscales": jnp.clip(jnp.exp(jax.random.uniform(seeds[8], (F,), jnp.float32, math.log(1.6), math.log(24.0))), 1.6, 24.0),
        "hypers": jnp.clip(jnp.exp(jax.random.uniform(seeds[9], (2,), jnp.float32, math.log(0.5), math.log(2.0))), 0.5, 2.0),
    }


def cross_cov(inducing, points, lengthscales, signal):
    scaled_z = inducing / lengthscales
    scaled_x = points.astype(jnp.float32) / lengthscales
    norm_z = jnp.sum(scaled_z * scaled_z, axis=1)
    norm_x = jnp.sum(scaled_x * scaled_x, axis=1)
    inner = jnp.dot(scaled_z, scaled_x.T, precision=lax.Precision.HIGHEST)
    return (signal * jnp.exp(-0.5 * (norm_z[:, None] + norm_x[None, :] - 2.0 * inner))).astype(jnp.bfloat16)


def reference(points, targets, inducing, whitening, mean_v, covariance, precision, natural_one, lengthscales, hypers):
    signal = hypers[0]
    noise_var = hypers[1]
    total = points.shape[0]
    blocks = total // TOK_DEV
    point_blocks = points.reshape(blocks, TOK_DEV, F)
    target_blocks = targets.reshape(blocks, TOK_DEV)

    def accumulate(carry, pieces):
        gram, proj, fit_sum = carry
        block_pts, block_tgt = pieces
        cross = cross_cov(inducing, block_pts, lengthscales, signal)
        white = jnp.dot(whitening, cross, preferred_element_type=jnp.float32).astype(jnp.bfloat16)
        white_wide = white.astype(jnp.float32)
        pred_mean = jnp.dot(mean_v, white_wide, precision=lax.Precision.HIGHEST)
        sq_norm = jnp.sum(white_wide * white_wide, axis=0)
        resid = block_tgt - pred_mean
        fit_sum = fit_sum + jnp.sum(resid * resid + signal - sq_norm)
        proj = proj + jnp.dot(white_wide, block_tgt, precision=lax.Precision.HIGHEST)
        gram = gram + lax.dot_general(white, white, (((1,), (1,)), ((), ())), preferred_element_type=jnp.float32)
        return (gram, proj, fit_sum), None

    start = (jnp.zeros((M, M), jnp.float32), jnp.zeros((M,), jnp.float32), jnp.zeros((), jnp.float32))
    (gram, proj, fit_sum), unused = lax.scan(accumulate, start, (point_blocks, target_blocks))
    trace = jnp.sum(covariance * gram)
    expected_fit = -0.5 * jnp.log(2.0 * jnp.pi * noise_var) - (fit_sum + trace) / (2.0 * noise_var * total)
    precision_new = 0.5 * precision + 0.5 * (jnp.eye(M, dtype=jnp.float32) + gram / noise_var)
    natural_new = 0.5 * natural_one + 0.5 * proj / noise_var
    return precision_new, natural_new, expected_fit
```

```python
import math

import jax
import jax.numpy as jnp
from jax import lax
from jax.sharding import Mesh, PartitionSpec as P

LOG2E = math.log2(math.e)
CHUNKS = 2
CROSS_BYTES = 2**25
PLANE = ("dp", "row")


def split3(value):
    high = lax.reduce_precision(value, 8, 7)
    rest = value - high
    mid = lax.reduce_precision(rest, 8, 7)
    low = rest - mid
    return [part.astype(jnp.bfloat16) for part in (high, mid, low)]


def dot_t(left, right):
    return lax.dot_general(
        left, right, (((1,), (1,)), ((), ())), preferred_element_type=jnp.float32
    )


def sum_over(value, axes):
    for axis in axes:
        size, turn = lax.axis_size(axis), 1
        while turn < size:
            value = value + lax.ppermute(value, axis, [(q, q ^ turn) for q in range(size)])
            turn *= 2
    return value


def shards(
    points,
    targets,
    inducing,
    whitening,
    mean_v,
    covariance,
    precision,
    natural_one,
    lengthscales,
    hypers,
):
    signal = hypers[0]
    noise_var = hypers[1]
    own_rows, width = whitening.shape
    own_cols = covariance.shape[1]
    planes = lax.axis_size("ind")
    chips = lax.axis_size(PLANE)
    side = lax.axis_index("core")
    chip = lax.axis_index(PLANE)
    groups = chips // planes
    total = points.shape[0] * chips * 2
    features = points.shape[1]

    strip = own_cols // (CHUNKS * chips)
    mine = lax.dynamic_index_in_dim(
        whitening.reshape(groups, 2, CHUNKS, chips, strip, width), side, 1, keepdims=False
    )
    mine = lax.dynamic_index_in_dim(mine, chip, 2, keepdims=False)
    gathered = [
        lax.all_gather(mine[:, at], "ind", axis=0, tiled=True) for at in range(CHUNKS)
    ]

    points_t = jnp.concatenate([points] + [part[:, None] for part in split3(targets)], axis=1)
    half = lax.all_gather(points_t, PLANE, axis=0, tiled=True)
    half_points, half_targets = half[:, :features], half[:, features:]
    feats = jnp.concatenate([inducing, mean_v[:, None]], axis=1).T
    seat = own_rows // (2 * chips)
    feats = lax.dynamic_slice_in_dim(feats, (chip * 2 + side) * seat, seat, 1)
    feats = lax.all_gather(feats, "ind", axis=1)
    middle = feats.shape[0] // 2
    feats = jnp.concatenate(
        [
            lax.all_gather(part, PLANE + ("core",), axis=2).reshape(part.shape[0], -1)
            for part in (feats[:middle], feats[middle:])
        ],
        axis=0,
    )
    all_inducing = feats[:features]
    all_mean = feats[features]

    scale_in = lengthscales[:, None]
    scaled_z = all_inducing / scale_in
    norm_z = jnp.log2(signal) - (0.5 * LOG2E) * jnp.sum(scaled_z * scaled_z, axis=0)
    weights = split3((scaled_z / scale_in) * LOG2E)
    left = jnp.concatenate(
        weights
        + [part[None, :] for part in split3(norm_z)]
        + [jnp.ones((3, all_inducing.shape[1]), jnp.bfloat16)],
        axis=0,
    )
    scaled_x = half_points.astype(jnp.float32) / lengthscales
    norm_x = (-0.5 * LOG2E) * jnp.sum(scaled_x * scaled_x, axis=1)
    right = jnp.concatenate(
        [half_points] * 3
        + [jnp.ones((half_points.shape[0], 3), jnp.bfloat16)]
        + [part[:, None] for part in split3(norm_x)],
        axis=1,
    )

    def cross_of(block):
        args = lax.dot_general(
            left, block, (((0,), (1,)), ((), ())), preferred_element_type=jnp.float32
        )
        return jnp.exp2(args).astype(jnp.bfloat16)

    def white_of(weight, cross):
        white = jnp.dot(weight, cross, preferred_element_type=jnp.float32).astype(jnp.bfloat16)
        return lax.optimization_barrier(white)

    swap = [(0, 1), (1, 0)]

    def send(piece):
        gots = []
        for turn in range(1, chips):
            sent = lax.dynamic_index_in_dim(piece, chip ^ turn, 0)
            gots.append(lax.ppermute(sent, PLANE, [(q, q ^ turn) for q in range(chips)]))
        return gots

    def assemble(piece, gots):
        strips = jnp.zeros(piece.shape, piece.dtype)
        own = lax.dynamic_index_in_dim(piece, chip, 0)
        strips = lax.dynamic_update_slice_in_dim(strips, own, chip, 0)
        for turn, got in enumerate(gots, 1):
            strips = lax.dynamic_update_slice_in_dim(strips, got, chip ^ turn, 0)
        return strips.reshape(chips * strip, width)

    def both_of(strips):
        return jnp.concatenate([strips, lax.ppermute(strips, "core", swap)], axis=0)

    def block_terms(block, block_targets, ready=None):
        cross = cross_of(block)
        white = white_of(whitening, cross)
        if ready is None:
            gots, white = lax.optimization_barrier((send(gathered[0]), white))
            grams = []
            for at in range(CHUNKS):
                strips = both_of(assemble(gathered[at], gots))
                if at + 1 < CHUNKS:
                    strips, piece = lax.optimization_barrier((strips, gathered[at + 1]))
                    right_white = white_of(strips, cross)
                    gots, right_white = lax.optimization_barrier((send(piece), right_white))
                    gram = dot_t(white, right_white)
                else:
                    gram = dot_t(white, white_of(strips, cross))
                grams.append(gram)
        else:
            grams = [dot_t(white, white_of(weight, cross)) for weight in ready]
        proj = jnp.sum(
            jnp.dot(white, block_targets, preferred_element_type=jnp.float32), axis=1
        )
        size = chips * strip
        return [part[:, :size] for part in grams], [part[:, size:] for part in grams], proj

    count = half_points.shape[0]
    blocks = 1
    while 2 * width * (count // blocks) > CROSS_BYTES:
        blocks *= 2
    if blocks == 1:
        own_gram, other_gram, proj_part = block_terms(right, half_targets)
    else:
        ready = [both_of(assemble(piece, send(piece))) for piece in gathered]

        def step(carry, pieces):
            return jax.tree.map(jnp.add, carry, block_terms(*pieces, ready)), None

        pieces = (
            right.reshape(blocks, count // blocks, -1),
            half_targets.reshape(blocks, count // blocks, -1),
        )
        start = jax.tree.map(
            lambda leaf: jnp.zeros(leaf.shape, leaf.dtype),
            jax.eval_shape(block_terms, pieces[0][0], pieces[1][0], ready),
        )
        (own_gram, other_gram, proj_part), unused = lax.scan(step, start, pieces)

    got = [lax.ppermute(part, "core", swap) for part in other_gram]
    gram = jnp.concatenate([a + b for a, b in zip(own_gram, got)], axis=1)
    proj = proj_part + lax.ppermute(proj_part, "core", swap)

    first_row = lax.axis_index("ind") * own_rows
    col = chip * 2 + side
    row_ids = first_row + jnp.arange(own_rows, dtype=jnp.int32)
    col_ids = col * own_cols + jnp.arange(own_cols, dtype=jnp.int32)
    identity = (row_ids[:, None] == col_ids[None, :]).astype(jnp.float32)
    col_mean = lax.dynamic_slice_in_dim(all_mean, col * own_cols, own_cols, 0)
    quad = jnp.sum((covariance + mean_v[:, None] * col_mean[None, :] - identity) * gram)
    once = jnp.where(col == 0, -2.0 * jnp.sum(mean_v * proj), 0.0)
    squares = jnp.where(lax.axis_index("ind") == 0, jnp.sum(targets * targets), 0.0)
    local = (quad + once + squares).reshape(1)
    fit_all = sum_over(local, ("core",) + PLANE + ("ind",))[0] + signal * total
    expected_fit = -0.5 * jnp.log(2.0 * jnp.pi * noise_var) - fit_all / (2.0 * noise_var * total)
    precision_new = 0.5 * precision + 0.5 * (identity + gram / noise_var)
    natural_new = 0.5 * natural_one + 0.5 * proj / noise_var
    return (precision_new, natural_new, expected_fit)


def solution(mesh):
    sizes = mesh.shape
    names = ("dp", "row", "core", "ind")
    pairs = Mesh(
        mesh.devices.reshape(sizes["dp"], sizes["rep"] // 2, 2, sizes["ind"]), names
    )
    cols = ("dp", "row", "core")
    return jax.shard_map(
        shards,
        mesh=pairs,
        in_specs=(
            P(cols, None),
            P(cols),
            P("ind", None),
            P("ind", None),
            P("ind"),
            P("ind", cols),
            P("ind", cols),
            P("ind"),
            P(),
            P(),
        ),
        out_specs=(P("ind", cols), P("ind"), P()),
        check_vma=False,
    )
```
